32 devices in a mesh: groups: 2 (over y), ctx: 4 (over z), head: 2 (over x), rep: 2 (over core).
Axes of the slice: x: 2, y: 2, z: 4, core: 2. Of those that a mesh axis runs over, the one named last changes fastest.
Arguments:
- kv_cache: bfloat16 [4, 96, 128, 576], P(('groups', 'rep'), 'ctx'), parts along dimension 0, may hold values from -10 to 10
- queries: bfloat16 [4, 4, 128, 576], P(('groups', 'rep'), None, 'head'), parts along dimension 0, may hold values from -45 to 45
- new_latent: bfloat16 [4, 4, 576], P(('groups', 'rep')), parts along dimension 0, may hold values from -6 to 6
- page_counts: int32 [4, 4], P(('groups', 'rep')), parts along dimension 0, may hold values from 1 to 36, 72 in all within a row
- page_tails: int32 [4, 4], P(('groups', 'rep')), parts along dimension 0, may hold values from 1 to 128
- page_slots: int32 [4, 96], P(('groups', 'rep')), parts along dimension 0, may hold values from 0 to 95, each once within a row
Outputs:
- attended: bfloat16 [4, 4, 128, 512], P(('groups', 'rep'), None, 'head'), parts along dimension 0
The draws below stay inside these ranges and needn't reach their ends.
There are 2 independent parts, one for each index of `groups`. The reference program is written for one: setup_inputs(seed, part) draws one part's arguments, and reference() takes and returns one part's arrays. A program takes and returns all parts, laid end to end along the dimension named above; each array names one. Nothing has to cross between parts.
Inputs may be any that keep to these rules, and one draw needn't show every extreme that they name: `page_counts`: the 4 counts of a half sum to 72, and the largest is exactly 36. `page_slots`: each half's row holds every slot once; only its first 72 entries are pages in use.
All inputs are finite; a program needn't handle non-finite values.
Results may differ from the reference program's by a relative error of at most 0.0033.
Values sent between devices are 32-bit elements; how exact they have to be, the bound alone decides.
A program may use at most 64 MiB of HBM per device.

```python
import math
import jax
import jax.numpy as jnp
import numpy as np
from jax import lax

HEADS = 128
LATENT = 512
PAGE = 128
BATCH = 4
KVW = 576
CTX_SLOTS = 96
TOTAL_PAGES = 72
MAXPAGES = 36
N_REP = 2


def draw_kv_cache(key, part):
    base = jnp.clip(jax.random.normal(jax.random.fold_in(key, 3), (N_REP, CTX_SLOTS, PAGE, KVW), jnp.float32), -6.0, 6.0)
    return base.astype(jnp.bfloat16)


def draw_queries(key, part):
    base = jnp.clip(jax.random.normal(jax.random.fold_in(key, 7), (N_REP, BATCH, HEADS, KVW), jnp.float32), -6.0, 6.0)
    return base.astype(jnp.bfloat16)


def plant(values, stream_key, low, largest):
    dims = values.shape
    place = [jax.random.randint(jax.random.fold_in(stream_key, axis), (), 0, dims[axis]) for axis in range(len(dims))]
    values = values.at[tuple(place)].set(low)
    longest = dims.index(max(dims))
    place[longest] = (place[longest] + 1) % dims[longest]
    return values.at[tuple(place)].set(largest)


def block_levels(own_key, shape, shards, low, high):
    def one(axis_at, shards_of):
        steps = jax.random.uniform(jax.random.fold_in(jax.random.fold_in(own_key, 6), axis_at), (shards_of,), jnp.float32, low / len(shards), high / len(shards))
        return jnp.repeat(jnp.exp(steps), shape[axis_at] // shards_of).reshape((-1,) + (1,) * (len(shape) - axis_at - 1))

    loudness = one(*shards[0])
    for cut in shards[1:]:
        loudness = loudness * one(*cut)
    return loudness


def length_profile(number_of, total, limit, skew):
    portions = [(1 << 20) // math.isqrt(rank ** skew) + 1 for rank in range(2, number_of + 1)]
    spare, given = total - limit - (number_of - 1), [1] * (number_of - 1)
    while spare > 0:
        movable = [i for i in range(number_of - 1) if given[i] < limit]
        whole, left = sum([portions[i] for i in movable]), spare
        for i in movable:
            more = min(limit - given[i], max(1, left * portions[i] // whole), spare)
            given[i] = given[i] + more
            spare = spare - more
    return np.array([limit] + given)


def ragged_sizes(key, count, total, reach, lean):
    if count == 2:
        one = jax.random.randint(key, (), max(1, total - reach), min(reach, total - 1) + 1)
        return jnp.stack([one, total - one])
    sizes = jnp.asarray(length_profile(count, total, reach, lean), jnp.int32)
    twos = (count - 1) // 2
    source_of, taker = sizes[1:1 + 2 * twos:2], sizes[2:2 + 2 * twos:2]
    margin = jnp.minimum(source_of - 1, reach - taker)
    moved = jax.random.randint(jax.random.fold_in(key, 1), (twos,), 0, 1 << 20) % (margin + 1)
    sizes = sizes.at[1:1 + 2 * twos:2].set(source_of - moved).at[2:2 + 2 * twos:2].set(taker + moved)
    return sizes[jax.random.permutation(jax.random.fold_in(key, 2), count)]


def gaussian(own_key, extent, width, limit, pieces=(), kind=jnp.bfloat16):
    level = block_levels(own_key, extent, pieces, -0.22, 0.18) if pieces else 1.0
    values = jax.random.normal(own_key, extent, jnp.float32) * width * level
    return jnp.minimum(jnp.maximum(values, -limit), limit).astype(kind)


def setup_inputs(seed: int = 0, part: int = 0) -> dict:
    key_list = jax.random.split(jax.random.key(seed), 7)
    part_keys = jax.random.split(jax.random.fold_in(key_list[6], part), 7)
    return {
        "kv_cache": draw_kv_cache(jax.random.fold_in(jax.random.fold_in(key_list[6], part), 71), part),
        "queries": draw_queries(jax.random.fold_in(jax.random.fold_in(key_list[6], part), 71), part),
        "new_latent": gaussian(part_keys[2], (N_REP, BATCH, KVW), 1.0, 6.0, ((0, 2),)),
        "page_counts": jax.vmap(lambda own: ragged_sizes(own, BATCH, TOTAL_PAGES, MAXPAGES, 2))(jax.random.split(part_keys[3], N_REP)).reshape((N_REP, BATCH)).astype(jnp.int32),
        "page_tails": plant(jax.random.randint(part_keys[4], (N_REP, BATCH), 1, PAGE + 1), jax.random.fold_in(part_keys[4], 1), 1, PAGE).astype(jnp.int32),
        "page_slots": jax.vmap(lambda own: jax.random.permutation(own, CTX_SLOTS))(jax.random.split(part_keys[5], N_REP)).reshape((N_REP, CTX_SLOTS)).astype(jnp.int32),
    }


score_scale = 192.0 ** -0.5
neg_large = -1.0e30


def page_partials(query_pages, cache_pages, token_valid):
    scores = jnp.einsum("phc,ptc->pht", query_pages.astype(jnp.float32), cache_pages.astype(jnp.float32)) * score_scale
    masked = jnp.where(token_valid[:, None, :], scores, neg_large)
    page_max = jnp.max(masked, axis=2)
    weights = jnp.where(token_valid[:, None, :], jnp.exp(masked - page_max[:, :, None]), 0.0).astype(jnp.bfloat16)
    page_sum = jnp.sum(weights.astype(jnp.float32), axis=2)
    page_acc = jnp.einsum("pht,ptc->phc", weights.astype(jnp.float32), cache_pages[:, :, :LATENT].astype(jnp.float32))
    return page_max, page_sum, page_acc


def reference(kv_cache, queries, new_latent, page_counts, page_tails, page_slots):
    halves = []
    for half in range(N_REP):
        counts = page_counts[half]
        ends = jnp.cumsum(counts).astype(jnp.int32)
        starts = (ends - counts).astype(jnp.int32)
        lengths = ((counts - 1) * PAGE + page_tails[half]).astype(jnp.int32)
        cache_half = kv_cache[half]
        slots_half = page_slots[half]

        def one_sequence(index):
            page_index = jnp.arange(MAXPAGES, dtype=jnp.int32)
            page_ok = page_index < jnp.take(counts, index)
            ranks = jnp.clip(jnp.take(starts, index) + page_index, 0, CTX_SLOTS - 1).astype(jnp.int32)
            slots = jnp.take(slots_half, ranks).astype(jnp.int32)
            cache_pages = jnp.take(cache_half, slots, axis=0)
            token_place = page_index[:, None] * PAGE + jnp.arange(PAGE, dtype=jnp.int32)[None, :]
            token_valid = page_ok[:, None] & (token_place < jnp.take(lengths, index))
            query_rows = queries[half][index]
            query_pages = jnp.broadcast_to(query_rows[None], (MAXPAGES,) + query_rows.shape)
            page_max, page_sum, page_acc = page_partials(query_pages, cache_pages, token_valid)
            own_row = new_latent[half][index].astype(jnp.float32)
            own_score = jnp.sum(query_rows.astype(jnp.float32) * own_row[None, :], axis=1) * score_scale
            top = jnp.maximum(jnp.max(page_max, axis=0), own_score)
            factor = jnp.exp(page_max - top[None, :])
            own_factor = jnp.exp(own_score - top)
            numer = jnp.sum(factor[:, :, None] * page_acc, axis=0) + own_factor[:, None] * own_row[None, :LATENT]
            denom = jnp.sum(factor * page_sum, axis=0) + own_factor
            return (numer / denom[:, None]).astype(jnp.bfloat16)

        halves.append(lax.map(one_sequence, jnp.arange(BATCH, dtype=jnp.int32)))
    return jnp.stack(halves)
```

```python
import functools
import math

import jax
import jax.numpy as jnp
from jax import lax
from jax.experimental import pallas as pl
from jax.experimental.pallas import tpu as pltpu
from jax.sharding import PartitionSpec as P

LATENT = 512
SCALE = 192.0 ** (-0.5) * math.log2(math.e)
NEG = -1e30
PIECES = 4
LAG = 6
MESH = pl.DeviceIdType.MESH


def kernel(
    n,
    counts_hbm,
    tails_hbm,
    slots_hbm,
    latent_hbm,
    q_hbm,
    kv_hbm,
    out_ref,
    counts_ref,
    tails_ref,
    slots_ref,
    latent_ref,
    q_v,
    kv_v,
    own_v,
    bias_v,
    score_v,
    weight_v,
    acc_v,
    inbox,
    part_v,
    cross,
    total_v,
    final,
    stat_out,
    stat_in,
    load_sem,
    small_sem,
    stat_send,
    stat_recv,
    in_send,
    in_recv,
    cross_recv,
    fin_send,
    fin_recv,
):
    batch, rows, width = q_v.shape
    pages, _, page = kv_hbm.shape[1:]
    tokens = pages * page
    slots = slots_hbm.shape[1]
    me = lax.axis_index("ctx")
    half = n // 2
    left = me < half
    inward = jnp.where(left, me + 1, me - 1)
    outward = jnp.where(left, me - 1, me + 1)
    is_end = (me == 0) | (me == n - 1)
    is_mid = (me == half - 1) | (me == half)
    inner = jnp.logical_not(is_end)

    smalls = [
        pltpu.make_async_copy(source, target, small_sem.at[i])
        for i, (source, target) in enumerate(
            [
                (counts_hbm, counts_ref),
                (tails_hbm, tails_ref),
                (slots_hbm, slots_ref),
                (latent_hbm, latent_ref),
            ]
        )
    ]
    for small in smalls:
        small.start()
    loads = [pltpu.make_async_copy(q_hbm.at[0], q_v, load_sem.at[pages])]
    for i in range(pages):
        loads.append(
            pltpu.make_async_copy(
                kv_hbm.at[0, i],
                kv_v.at[:, pl.ds(i * page, page)],
                load_sem.at[i],
            )
        )
    for load in loads:
        load.start()

    barrier = pltpu.get_barrier_semaphore()

    @pl.loop(1, n)
    def _(off):
        pl.semaphore_signal(
            barrier, inc=1, device_id={"ctx": lax.rem(me + off, n)}, device_id_type=MESH
        )

    for small in smalls:
        small.wait()
    own_v[...] = jnp.zeros((page, width), jnp.bfloat16)
    own_v[0:batch, :] = latent_ref[0]

    slot_id = me * pages + lax.broadcasted_iota(jnp.int32, (pages, slots), 0)
    rank = lax.broadcasted_iota(jnp.int32, (pages, slots), 1)
    match = slots_ref[...] == slot_id
    lane = lax.broadcasted_iota(jnp.int32, (pages, page), 1)
    lane_own = lax.broadcasted_iota(jnp.int32, (8, page), 1)
    begin = jnp.int32(0)
    for s in range(batch):
        count = counts_ref[0, s]
        length = (count - 1) * page + tails_ref[0, s]
        place = rank - begin
        inside = match & (place >= 0) & (place < count)
        limit = jnp.sum(
            jnp.where(inside, (length - place * page).astype(jnp.float32), 0.0),
            axis=1,
            keepdims=True,
        )
        bias_v[s, 0:pages, :] = jnp.where(lane.astype(jnp.float32) < limit, 0.0, NEG)
        own_here = (lane_own == s) & (me == 0)
        bias_v[s, pages : pages + 8, :] = jnp.where(own_here, 0.0, NEG)
        begin = begin + count

    loads[0].wait()
    queries = q_v[...].reshape(batch * rows, width)
    tops = [jnp.full((rows, page), NEG, jnp.float32) for _ in range(batch)]
    nt = (((1,), (1,)), ((), ()))
    for first in [*range(0, pages, 2), pages]:
        many = min(2, pages - first) or 1
        if first < pages:
            for j in range(many):
                loads[1 + first + j].wait()
            keys = kv_v[:, first * page : (first + many) * page]
            block = jnp.dot(queries, keys, preferred_element_type=jnp.float32)
        else:
            block = lax.dot_general(
                queries, own_v[...], nt, preferred_element_type=jnp.float32
            )
        for s in range(batch):
            for j in range(many):
                at = first + j
                value = (
                    block[s * rows : (s + 1) * rows, j * page : (j + 1) * page] * SCALE
                    + bias_v[s, at : at + 1, :]
                )
                score_v[s, :, at * page : (at + 1) * page] = value
                tops[s] = jnp.maximum(tops[s], value)

    size = batch * rows // PIECES
    wide = out_ref.shape[3] // page

    def piece(k):
        return k // PIECES, pl.ds((k % PIECES) * size, size)

    def ship(source, target, send, recv, k, to):
        s, at = piece(k)
        return pltpu.make_async_remote_copy(
            src_ref=source.at[s, at],
            dst_ref=target.at[s, at],
            send_sem=send.at[k],
            recv_sem=recv.at[k],
            device_id={"ctx": to},
            device_id_type=MESH,
        )

    def stat_copy(s, to, origin, slot):
        return pltpu.make_async_remote_copy(
            src_ref=stat_out.at[s],
            dst_ref=stat_in.at[s, origin],
            send_sem=stat_send.at[s, slot],
            recv_sem=stat_recv.at[s, origin],
            device_id={"ctx": to},
            device_id_type=MESH,
        )

    def other(off):
        to = lax.rem(me + off, n)
        return to, (to > 0) & (to < n - 1)

    lane_row = lax.broadcasted_iota(jnp.int32, (rows, page), 1)
    for s in range(batch):
        top = jnp.max(tops[s], axis=1, keepdims=True)
        total = jnp.zeros((rows, page), jnp.float32)
        for at in range(pages + 1):
            cols = slice(at * page, (at + 1) * page)
            weight = jnp.exp2(score_v[s, :, cols] - top).astype(jnp.bfloat16)
            weight_v[s * rows : (s + 1) * rows, cols] = weight
            total = total + weight.astype(jnp.float32)
        total = jnp.sum(total, axis=1, keepdims=True)
        pair = jnp.where(lane_row == 0, top, total)
        square = jnp.concatenate([pair] * (page // rows), axis=0)
        tile = jnp.transpose(square)[0:8]
        stat_out[s] = tile
        stat_in[s, pl.ds(me, 1)] = tile[None]
        if s == 0:
            pl.semaphore_wait(barrier, n - 1)

        @pl.loop(1, n)
        def _(off):
            to, wanted = other(off)

            @pl.when(wanted)
            def _():
                stat_copy(s, to, me, off).start()

    group = 2
    for j in range(0, wide, group):
        span = slice(j * page, (j + group) * page)
        block = lax.dot_general(
            weight_v[:, 0:tokens], kv_v[span, :], nt, preferred_element_type=jnp.float32
        ) + jnp.dot(
            weight_v[:, tokens:], own_v[:, span], preferred_element_type=jnp.float32
        )
        for i in range(group):
            acc_v[j + i] = block[:, i * page : (i + 1) * page]

        @pl.when(is_end)
        def _():
            for k in range(j * PIECES, (j + group) * PIECES):
                ship(acc_v, inbox, in_send, in_recv, k, inward).start()

    def emit(k, value):
        j = k // PIECES
        first = (k % PIECES) * size
        value = value.astype(jnp.bfloat16)
        for lo in range(0, size, min(size, rows)):
            s, r = divmod(first + lo, rows)
            out_ref[0, s, r : r + min(size, rows), j * page : (j + 1) * page] = value[
                lo : lo + min(size, rows)
            ]

    number = wide * PIECES
    from_end = (outward == 0) | (outward == n - 1)

    def factors(s):
        @pl.loop(1, n)
        def _(off):
            stat_copy(s, me, lax.rem(me + off, n), off).wait_recv()

        best = stat_in[s, 0]
        for j in range(1, n):
            best = jnp.maximum(best, stat_in[s, j])
        best = best[0:1]
        denom = jnp.zeros((1, page), jnp.float32)
        mine = jnp.zeros((1, page), jnp.float32)
        theirs = jnp.zeros((1, page), jnp.float32)
        for j in range(n):
            tile = stat_in[s, j]
            keep = jnp.exp2(tile[0:1] - best)
            denom = denom + keep * tile[1:2]
            mine = jnp.where(me == j, keep, mine)
            theirs = jnp.where(outward == j, keep, theirs)
        mine = mine / denom
        theirs = jnp.where(from_end, theirs / denom, 1.0)
        row = lax.broadcasted_iota(jnp.int32, (page, page), 0)
        turned = jnp.transpose(jnp.where(row == 0, mine, theirs))
        return turned[0:rows, 0:1], turned[0:rows, 1:2]

    @pl.when(inner)
    def _():
        pairs = [factors(s) for s in range(batch)]
        scales = [jnp.concatenate(f, axis=0) for f in zip(*pairs)]
        for k in range(number + LAG):
            if k < number:
                s, at = piece(k)
                lo = (k % PIECES) * size
                mine, theirs = (f[lo : lo + size] for f in scales)
                ship(acc_v, inbox, in_send, in_recv, k, inward).wait_recv()
                part_v[s, at] = acc_v[s, at] * mine + inbox[s, at] * theirs

                @pl.when(is_mid)
                def _():
                    ship(part_v, cross, in_send, cross_recv, k, inward).start()

                @pl.when(jnp.logical_not(is_mid))
                def _():
                    ship(part_v, inbox, in_send, in_recv, k, inward).start()

            if k >= LAG:
                d = k - LAG
                s, at = piece(d)

                @pl.when(is_mid)
                def _():
                    ship(part_v, cross, in_send, cross_recv, d, inward).wait_recv()
                    total = part_v[s, at] + cross[s, at]
                    total_v[s, at] = total
                    ship(total_v, final, fin_send, fin_recv, d, outward).start()
                    emit(d, total)

                @pl.when(jnp.logical_not(is_mid))
                def _():
                    ship(final, final, fin_send, fin_recv, d, outward).wait_recv()
                    ship(final, final, fin_send, fin_recv, d, outward).start()
                    emit(d, final[s, at])

        for k in range(number):
            ship(total_v, final, fin_send, fin_recv, k, outward).wait_send()

    @pl.when(is_end)
    def _():
        for k in range(number):
            s, at = piece(k)
            ship(total_v, final, fin_send, fin_recv, k, inward).wait_recv()
            emit(k, final[s, at])

    for k in range(number):
        ship(part_v, inbox, in_send, in_recv, k, inward).wait_send()
    for s in range(batch):

        @pl.loop(1, n)
        def _(off):
            to, wanted = other(off)

            @pl.when(wanted)
            def _():
                stat_copy(s, to, me, off).wait_send()


def local(n, kv_cache, queries, new_latent, page_counts, page_tails, page_slots):
    _, pages, page, width = kv_cache.shape
    _, batch, rows, _ = queries.shape
    number = LATENT // page * PIECES
    block = (LATENT // page, batch * rows, page)
    hbm = pl.BlockSpec(memory_space=pltpu.HBM)
    dma = pltpu.SemaphoreType.DMA
    return pl.pallas_call(
        functools.partial(kernel, n),
        out_shape=pltpu.VMEM((1, batch, rows, LATENT), jnp.bfloat16),
        in_specs=[hbm] * 6,
        scratch_shapes=[
            pltpu.SMEM(page_counts.shape, jnp.int32),
            pltpu.SMEM(page_tails.shape, jnp.int32),
            pltpu.VMEM(page_slots.shape, jnp.int32),
            pltpu.VMEM(new_latent.shape, jnp.bfloat16),
            pltpu.VMEM((batch, rows, width), jnp.bfloat16),
            pltpu.VMEM((width, pages * page), jnp.bfloat16),
            pltpu.VMEM((page, width), jnp.bfloat16),
            pltpu.VMEM((batch, pages + 8, page), jnp.float32),
            pltpu.VMEM((batch, rows, (pages + 1) * page), jnp.float32),
            pltpu.VMEM((batch * rows, (pages + 1) * page), jnp.bfloat16),
            pltpu.VMEM(block, jnp.float32),
            pltpu.VMEM(block, jnp.float32),
            pltpu.VMEM(block, jnp.float32),
            pltpu.VMEM(block, jnp.float32),
            pltpu.VMEM(block, jnp.float32),
            pltpu.VMEM(block, jnp.float32),
            pltpu.VMEM((batch, 8, page), jnp.float32),
            pltpu.VMEM((batch, n, 8, page), jnp.float32),
            dma((pages + 1,)),
            dma((4,)),
            dma((batch, n)),
            dma((batch, n)),
            dma((number,)),
            dma((number,)),
            dma((number,)),
            dma((number,)),
            dma((number,)),
        ],
        compiler_params=pltpu.CompilerParams(
            collective_id=0, has_side_effects=True
        ),
    )(page_counts, page_tails, page_slots, new_latent, queries, jnp.swapaxes(kv_cache, 2, 3))


def solution(mesh):
    in_specs = (
        P(("groups", "rep"), "ctx", None, None),
        P(("groups", "rep"), None, "head", None),
        P(("groups", "rep"), None, None),
        P(("groups", "rep"), None),
        P(("groups", "rep"), None),
        P(("groups", "rep"), None),
    )
    out_specs = P(("groups", "rep"), None, "head", None)
    return jax.shard_map(
        functools.partial(local, mesh.shape["ctx"]),
        mesh=mesh,
        in_specs=in_specs,
        out_specs=out_specs,
        check_vma=False,
    )
```

```python
import functools
import math

import jax
import jax.numpy as jnp
from jax import lax
from jax.experimental import pallas as pl
from jax.experimental.pallas import tpu as pltpu
from jax.sharding import PartitionSpec as P

LATENT = 512
SCALE = 192.0 ** (-0.5) * math.log2(math.e)
NEG = -1e30
PIECE = 64
TAIL = ()
LAG = 6
CHUNKS = 1
MESH = pl.DeviceIdType.MESH


def cut(total):
    sizes = list(TAIL) if total > sum(TAIL) else []
    while sum(sizes) < total:
        sizes.insert(0, min(PIECE, total - sum(sizes)))
    return [(sum(sizes[:k]), size) for k, size in enumerate(sizes)]


def kernel(
    n,
    counts_hbm,
    tails_hbm,
    slots_hbm,
    latent_hbm,
    q_hbm,
    kv_hbm,
    out_ref,
    counts_ref,
    tails_ref,
    slots_ref,
    latent_ref,
    q_v,
    kv_v,
    own_v,
    bias_v,
    score_v,
    weight_v,
    acc_v,
    inbox,
    part_v,
    inner_box,
    total_v,
    stat_out,
    stat_in,
    small_sem,
    q_sem,
    kv_sem,
    stat_send,
    stat_recv,
    send_sem,
    out_recv,
    in_recv,
):
    batch, rows, width = q_v.shape
    pages, _, page = kv_v.shape
    tokens = pages * page
    slots = slots_ref.shape[1]
    height = batch * rows
    groups, many = stat_out.shape[0], page // rows
    wide = LATENT // page
    pieces = cut(wide * height)
    number = len(pieces)
    me = lax.axis_index("ctx")
    half = n // 2
    left = me < half
    inward = jnp.where(left, me + 1, me - 1)
    outward = jnp.where(left, me - 1, me + 1)
    is_end = (me == 0) | (me == n - 1)
    is_mid = (me == half - 1) | (me == half)
    inner = jnp.logical_not(is_end)
    all_mid = n <= 4

    smalls = [
        pltpu.make_async_copy(source, target, small_sem.at[i])
        for i, (source, target) in enumerate(
            [
                (counts_hbm, counts_ref),
                (tails_hbm, tails_ref),
                (slots_hbm, slots_ref),
                (latent_hbm, latent_ref),
            ]
        )
    ]
    for small in smalls:
        small.start()
    q_load = pltpu.make_async_copy(q_hbm.at[0], q_v, q_sem)
    q_load.start()
    step = pages // CHUNKS
    loads = []
    for i in range(CHUNKS):
        at = pl.ds(i * step, step)
        loads.append(
            pltpu.make_async_copy(kv_hbm.at[0, at], kv_v.at[at], kv_sem.at[i])
        )
        loads[-1].start(priority=1)

    barrier = pltpu.get_barrier_semaphore()

    @pl.loop(1, n)
    def _(off):
        pl.semaphore_signal(
            barrier, inc=1, device_id={"ctx": lax.rem(me + off, n)}, device_id_type=MESH
        )

    for small in smalls:
        small.wait()
    own_v[...] = jnp.zeros((page, width), jnp.bfloat16)
    own_v[0:batch, :] = latent_ref[0]

    slot_id = me * pages + lax.broadcasted_iota(jnp.int32, (pages, slots), 0)
    rank = lax.broadcasted_iota(jnp.int32, (pages, slots), 1)
    match = slots_ref[...] == slot_id
    lane = lax.broadcasted_iota(jnp.int32, (pages, page), 1)
    lane_own = lax.broadcasted_iota(jnp.int32, (8, page), 1)
    begin = jnp.int32(0)
    for s in range(batch):
        count = counts_ref[0, s]
        length = (count - 1) * page + tails_ref[0, s]
        place = rank - begin
        inside = match & (place >= 0) & (place < count)
        limit = jnp.sum(
            jnp.where(inside, (length - place * page).astype(jnp.float32), 0.0),
            axis=1,
            keepdims=True,
        )
        bias_v[s, 0:pages, :] = jnp.where(lane.astype(jnp.float32) < limit, 0.0, NEG)
        own_here = (lane_own == s) & (me == 0)
        bias_v[s, pages : pages + 8, :] = jnp.where(own_here, 0.0, NEG)
        begin = begin + count

    q_load.wait()
    queries = q_v[...].reshape(height, width)
    tops = [jnp.full((rows, page), NEG, jnp.float32) for _ in range(batch)]
    nt = (((1,), (1,)), ((), ()))
    for first in range(0, pages + 1, 2):
        two = min(2, pages + 1 - first)
        if first < pages:
            if first % step == 0:
                loads[first // step].wait()
            keys = jnp.concatenate([kv_v[first + j] for j in range(two)], axis=1)
            block = jnp.dot(queries, keys, preferred_element_type=jnp.float32)
        else:
            block = lax.dot_general(
                queries, own_v[...], nt, preferred_element_type=jnp.float32
            )
        for s in range(batch):
            for j in range(two):
                at = first + j
                value = (
                    block[s * rows : (s + 1) * rows, j * page : (j + 1) * page] * SCALE
                    + bias_v[s, at : at + 1, :]
                )
                score_v[at, s * rows : (s + 1) * rows, :] = value
                tops[s] = jnp.maximum(tops[s], value)

    tops = [jnp.max(top, axis=1, keepdims=True) for top in tops]
    totals = [jnp.zeros((rows, page), jnp.float32) for _ in range(batch)]
    for at in range(pages + 1):
        for s in range(batch):
            span = slice(s * rows, (s + 1) * rows)
            weight = jnp.exp2(score_v[at, span, :] - tops[s]).astype(jnp.bfloat16)
            weight_v[span, at * page : (at + 1) * page] = weight
            totals[s] = totals[s] + weight.astype(jnp.float32)

    def attend(first, blocks):
        span = slice(first * page, (first + blocks) * page)
        values = jnp.concatenate([kv_v[i, span, :] for i in range(pages)], axis=1)
        block = lax.dot_general(
            weight_v[:, 0:tokens], values, nt, preferred_element_type=jnp.float32
        ) + jnp.dot(
            weight_v[:, tokens:], own_v[:, span], preferred_element_type=jnp.float32
        )
        for i in range(blocks):
            acc_v[(first + i) * height : (first + i + 1) * height, :] = block[
                :, i * page : (i + 1) * page
            ]

    def ship(source, target, send, recv, k, to):
        at = pl.ds(*pieces[k])
        return pltpu.make_async_remote_copy(
            src_ref=source.at[at],
            dst_ref=target.at[at],
            send_sem=send_sem.at[send],
            recv_sem=recv.at[k],
            device_id={"ctx": to},
            device_id_type=MESH,
        )

    def to_inbox(source, k):
        return ship(source, inbox, 0, out_recv, k, inward)

    def to_mid(k):
        return ship(part_v, inner_box, 0, in_recv, k, inward)

    def to_out(source, k):
        return ship(source, inner_box, 1, in_recv, k, outward)

    def stat_copy(to, origin, slot):
        return pltpu.make_async_remote_copy(
            src_ref=stat_out,
            dst_ref=stat_in.at[origin],
            send_sem=stat_send.at[slot],
            recv_sem=stat_recv.at[origin],
            device_id={"ctx": to},
            device_id_type=MESH,
        )

    def other(off):
        to = lax.rem(me + off, n)
        return to, (to > 0) & (to < n - 1)

    lane_row = lax.broadcasted_iota(jnp.int32, (rows, page), 1)
    for g in range(groups):
        pairs = [
            jnp.where(lane_row == 0, tops[s], jnp.sum(totals[s], axis=1, keepdims=True))
            for s in range(g * many, (g + 1) * many)
        ]
        tile = jnp.transpose(jnp.concatenate(pairs, axis=0))[0:8]
        stat_out[g] = tile
        stat_in[pl.ds(me, 1), g] = tile[None]

    group = 2
    sent = 0
    for j in range(0, wide, group):
        attend(j, group)
        if j == 0:
            pl.semaphore_wait(barrier, n - 1)

            @pl.loop(1, n)
            def _(off):
                to, wanted = other(off)

                @pl.when(wanted)
                def _():
                    stat_copy(to, me, off).start()

        ready = [
            k for k in range(sent, number) if sum(pieces[k]) <= (j + group) * height
        ]
        sent += len(ready)

        @pl.when(is_end)
        def _():
            for k in ready:
                to_inbox(acc_v, k).start()

    def emit(k, value):
        value = value.astype(jnp.bfloat16)
        first, size = pieces[k]
        lo = first
        while lo < first + size:
            j, at = divmod(lo, height)
            s, r = divmod(at, rows)
            take = min(rows - r, first + size - lo)
            out_ref[0, s, r : r + take, j * page : (j + 1) * page] = value[
                lo - first : lo - first + take
            ]
            lo += take

    from_end = (outward == 0) | (outward == n - 1)

    def factors(g):
        best = stat_in[0, g]
        for j in range(1, n):
            best = jnp.maximum(best, stat_in[j, g])
        best = best[0:1]
        denom = jnp.zeros((1, page), jnp.float32)
        mine = jnp.zeros((1, page), jnp.float32)
        theirs = jnp.zeros((1, page), jnp.float32)
        for j in range(n):
            tile = stat_in[j, g]
            keep = jnp.exp2(tile[0:1] - best)
            denom = denom + keep * tile[1:2]
            mine = jnp.where(me == j, keep, mine)
            theirs = jnp.where(outward == j, keep, theirs)
        mine = mine / denom
        theirs = jnp.where(from_end, theirs / denom, 1.0)
        row = lax.broadcasted_iota(jnp.int32, (page, page), 0)
        turned = jnp.transpose(jnp.where(row == 0, mine, theirs))
        return turned[:, 0:1], turned[:, 1:2]

    def rows_of(factor, k):
        first, size = pieces[k]
        parts = []
        lo = first
        while lo < first + size:
            at = lo % height
            take = min(height - at, first + size - lo)
            parts.append(factor[at : at + take])
            lo += take
        return parts[0] if len(parts) == 1 else jnp.concatenate(parts, axis=0)

    @pl.when(inner)
    def _():
        @pl.loop(1, n)
        def _(off):
            stat_copy(me, lax.rem(me + off, n), off).wait_recv()

        pairs = [factors(g) for g in range(groups)]
        scales = [jnp.concatenate(f, axis=0) for f in zip(*pairs)]
        for k in range(number + LAG):
            if k < number:
                at = pl.ds(*pieces[k])
                mine, theirs = (rows_of(f, k) for f in scales)
                to_inbox(acc_v, k).wait_recv()
                part_v[at] = acc_v[at] * mine + inbox[at] * theirs
                if all_mid:
                    to_mid(k).start()
                else:

                    @pl.when(is_mid)
                    def _():
                        to_mid(k).start()

                    @pl.when(jnp.logical_not(is_mid))
                    def _():
                        to_inbox(part_v, k).start()

            if k >= LAG:
                d = k - LAG
                at = pl.ds(*pieces[d])
                to_mid(d).wait_recv()

                def finish():
                    total = part_v[at] + inner_box[at]
                    total_v[at] = total
                    to_out(total_v, d).start()
                    emit(d, total)

                if all_mid:
                    finish()
                else:
                    pl.when(is_mid)(finish)

                    @pl.when(jnp.logical_not(is_mid))
                    def _():
                        to_out(inner_box, d).start()
                        emit(d, inner_box[at])

        pltpu.make_async_remote_copy(
            src_ref=total_v,
            dst_ref=inner_box,
            send_sem=send_sem.at[1],
            recv_sem=in_recv.at[0],
            device_id={"ctx": outward},
            device_id_type=MESH,
        ).wait_send()

    @pl.when(is_end)
    def _():
        for k in range(number):
            to_mid(k).wait_recv()
            emit(k, inner_box[pl.ds(*pieces[k])])

    pltpu.make_async_remote_copy(
        src_ref=part_v,
        dst_ref=inbox,
        send_sem=send_sem.at[0],
        recv_sem=out_recv.at[0],
        device_id={"ctx": inward},
        device_id_type=MESH,
    ).wait_send()

    @pl.loop(1, n)
    def _(off):
        to, wanted = other(off)

        @pl.when(wanted)
        def _():
            stat_copy(to, me, off).wait_send()


def local(n, kv_cache, queries, new_latent, page_counts, page_tails, page_slots):
    _, pages, page, width = kv_cache.shape
    _, batch, rows, _ = queries.shape
    height = batch * rows
    flat = (LATENT // page * height, page)
    number = len(cut(flat[0]))
    groups = height // page
    hbm = pl.BlockSpec(memory_space=pltpu.HBM)
    dma = pltpu.SemaphoreType.DMA
    return pl.pallas_call(
        functools.partial(kernel, n),
        out_shape=pltpu.VMEM((1, batch, rows, LATENT), jnp.bfloat16),
        in_specs=[hbm] * 6,
        scratch_shapes=[
            pltpu.SMEM(page_counts.shape, jnp.int32),
            pltpu.SMEM(page_tails.shape, jnp.int32),
            pltpu.VMEM(page_slots.shape, jnp.int32),
            pltpu.VMEM(new_latent.shape, jnp.bfloat16),
            pltpu.VMEM((batch, rows, width), jnp.bfloat16),
            pltpu.VMEM((pages, width, page), jnp.bfloat16),
            pltpu.VMEM((page, width), jnp.bfloat16),
            pltpu.VMEM((batch, pages + 8, page), jnp.float32),
            pltpu.VMEM((pages + 1, height, page), jnp.float32),
            pltpu.VMEM((height, (pages + 1) * page), jnp.bfloat16),
            pltpu.VMEM(flat, jnp.float32),
            pltpu.VMEM(flat, jnp.float32),
            pltpu.VMEM(flat, jnp.float32),
            pltpu.VMEM(flat, jnp.float32),
            pltpu.VMEM(flat, jnp.float32),
            pltpu.VMEM((groups, 8, page), jnp.float32),
            pltpu.VMEM((n, groups, 8, page), jnp.float32),
            dma((4,)),
            dma,
            dma((CHUNKS,)),
            dma((n,)),
            dma((n,)),
            dma((2,)),
            dma((number,)),
            dma((number,)),
        ],
        compiler_params=pltpu.CompilerParams(
            collective_id=0, has_side_effects=True
        ),
    )(page_counts, page_tails, page_slots, new_latent, queries, jnp.swapaxes(kv_cache, 2, 3))


def solution(mesh):
    in_specs = (
        P(("groups", "rep"), "ctx", None, None),
        P(("groups", "rep"), None, "head", None),
        P(("groups", "rep"), None, None),
        P(("groups", "rep"), None),
        P(("groups", "rep"), None),
        P(("groups", "rep"), None),
    )
    out_specs = P(("groups", "rep"), None, "head", None)
    return jax.shard_map(
        functools.partial(local, mesh.shape["ctx"]),
        mesh=mesh,
        in_specs=in_specs,
        out_specs=out_specs,
        check_vma=False,
    )
```

```python
import functools
import math

import jax
import jax.numpy as jnp
from jax import lax
from jax.experimental import pallas as pl
from jax.experimental.pallas import tpu as pltpu
from jax.sharding import PartitionSpec as P

LATENT = 512
SCALE = 192.0 ** (-0.5) * math.log2(math.e)
NEG = -1e30
PIECE = 32
HEAD = ()
LAG_LEFT = 320
LAG_RIGHT = 320
CHUNKS = 2
MESH = pl.DeviceIdType.MESH


def cut(total):
    sizes = list(HEAD) if total > sum(HEAD) else []
    while sum(sizes) < total:
        sizes.append(min(PIECE, total - sum(sizes)))
    return [(sum(sizes[:k]), size) for k, size in enumerate(sizes)]


def merge(pieces, lag):
    order = []
    k = d = 0
    while d < len(pieces):
        if k < len(pieces) and pieces[k][0] < pieces[d][0] + lag:
            order.append((k, None))
            k += 1
        else:
            order.append((None, d))
            d += 1
    return order


def kernel(
    n,
    counts_hbm,
    tails_hbm,
    slots_hbm,
    latent_hbm,
    q_hbm,
    kv_hbm,
    out_ref,
    counts_ref,
    tails_ref,
    slots_ref,
    latent_ref,
    q_v,
    kv_v,
    own_v,
    bias_v,
    owner_v,
    across_v,
    score_v,
    weight_v,
    acc_v,
    inbox,
    part_v,
    inner_box,
    total_v,
    stat_out,
    stat_in,
    small_sem,
    q_sem,
    kv_sem,
    stat_send,
    stat_recv,
    send_sem,
    out_recv,
    in_recv,
):
    batch, rows, width = q_v.shape
    pages, _, page = kv_v.shape
    tokens = pages * page
    slots = slots_ref.shape[1]
    height = batch * rows
    groups, many = stat_out.shape[0], page // rows
    wide = LATENT // page
    pieces = cut(wide * height)
    number = len(pieces)
    me = lax.axis_index("ctx")
    half = n // 2
    left = me < half
    inward = jnp.where(left, me + 1, me - 1)
    outward = jnp.where(left, me - 1, me + 1)
    is_end = (me == 0) | (me == n - 1)
    is_mid = (me == half - 1) | (me == half)
    inner = jnp.logical_not(is_end)
    all_mid = n <= 4

    smalls = [
        pltpu.make_async_copy(source, target, small_sem.at[i])
        for i, (source, target) in enumerate(
            [
                (counts_hbm, counts_ref),
                (tails_hbm, tails_ref),
                (slots_hbm, slots_ref),
                (latent_hbm, latent_ref),
            ]
        )
    ]
    for small in smalls:
        small.start()
    q_load = pltpu.make_async_copy(q_hbm.at[0], q_v, q_sem)
    q_load.start()
    step = pages // CHUNKS
    loads = []
    for i in range(CHUNKS):
        at = pl.ds(i * step, step)
        loads.append(
            pltpu.make_async_copy(kv_hbm.at[0, at], kv_v.at[at], kv_sem.at[i])
        )
        loads[-1].start(priority=1)

    barrier = pltpu.get_barrier_semaphore()

    @pl.loop(1, n)
    def _(off):
        pl.semaphore_signal(
            barrier, inc=1, device_id={"ctx": lax.rem(me + off, n)}, device_id_type=MESH
        )

    for small in smalls:
        small.wait()
    own_v[...] = jnp.zeros((page, width), jnp.bfloat16)
    own_v[0:batch, :] = latent_ref[0]

    slot_id = me * pages + lax.broadcasted_iota(jnp.int32, (pages, slots), 0)
    rank = lax.broadcasted_iota(jnp.int32, (pages, slots), 1)
    match = slots_ref[...] == slot_id
    lane = lax.broadcasted_iota(jnp.int32, (pages, page), 1)
    begin = jnp.int32(0)
    limits = jnp.zeros((pages, page), jnp.float32)
    table = jnp.zeros((pages, page), jnp.float32)
    for s in range(batch):
        count = counts_ref[0, s]
        length = (count - 1) * page + tails_ref[0, s]
        place = rank - begin
        inside = match & (place >= 0) & (place < count)
        limit = jnp.sum(
            jnp.where(inside, (length - place * page).astype(jnp.float32), 0.0),
            axis=1,
            keepdims=True,
        )
        limits = limits + limit
        table = jnp.where(lane == s, limit, table)
        owner_v[s, :, :] = jnp.where(limit > 0.0, jnp.ones((pages, page)), 0.0)
        begin = begin + count
    bias_v[...] = jnp.where(lane.astype(jnp.float32) < limits, 0.0, NEG)
    square = jnp.concatenate(
        [table, jnp.zeros((page - pages, page), jnp.float32)], axis=0
    )
    across_v[...] = jnp.transpose(square)[0:8]

    q_load.wait()
    queries = q_v[...].reshape(height, width)
    column = lax.broadcasted_iota(jnp.int32, (rows, page), 1)
    peaks = jnp.full((rows, page), NEG, jnp.float32)
    nt = (((1,), (1,)), ((), ()))

    def pick(at, parts):
        chosen = parts[-1]
        for s in reversed(range(batch - 1)):
            chosen = jnp.where(owner_v[s, at : at + 1, :] > 0.5, parts[s], chosen)
        return chosen

    def strips_of(block, j):
        cols = slice(j * page, (j + 1) * page)
        return [block[s * rows : (s + 1) * rows, cols] for s in range(batch)]

    block = lax.dot_general(queries, own_v[...], nt, preferred_element_type=jnp.float32)
    owns = [
        jnp.where((column == s) & (me == 0), strip * SCALE, NEG)
        for s, strip in enumerate(strips_of(block, 0))
    ]
    for first in range(0, pages, 2):
        two = min(2, pages - first)
        if first % step == 0:
            loads[first // step].wait()
        keys = jnp.concatenate([kv_v[first + j] for j in range(two)], axis=1)
        block = jnp.dot(queries, keys, preferred_element_type=jnp.float32)
        for j in range(two):
            at = first + j
            value = pick(at, strips_of(block, j)) * SCALE + bias_v[at : at + 1, :]
            score_v[at] = value
            peaks = jnp.where(
                column == at, jnp.max(value, axis=1, keepdims=True), peaks
            )

    tops = []
    for s in range(batch):
        held = jnp.where(across_v[s : s + 1, :] > 0.0, peaks, NEG)
        tops.append(jnp.max(jnp.maximum(held, owns[s]), axis=1, keepdims=True))
    spread = [jnp.broadcast_to(top, (rows, page)) for top in tops]
    sums = jnp.zeros((rows, page), jnp.float32)
    tiles = [(at, min(2, pages - at)) for at in range(0, pages, 2)] + [(pages, 1)]
    group = 2

    def attend(weights, first, at, count):
        span = slice(first * page, (first + group) * page)
        if at == pages:
            return jnp.dot(weights, own_v[:, span], preferred_element_type=jnp.float32)
        values = jnp.concatenate([kv_v[at + i, span, :] for i in range(count)], axis=1)
        return lax.dot_general(weights, values, nt, preferred_element_type=jnp.float32)

    def keep(first, block):
        for i in range(group):
            acc_v[(first + i) * height : (first + i + 1) * height, :] = block[
                :, i * page : (i + 1) * page
            ]

    block = None
    for at, count in tiles:
        if at == pages:
            strip = [
                jnp.exp2(own - top).astype(jnp.bfloat16)
                for own, top in zip(owns, spread)
            ]
            owns = [part.astype(jnp.float32) for part in strip]
            weights = jnp.concatenate(strip, axis=0)
        else:
            strips = []
            for i in range(at, at + count):
                weight = jnp.exp2(score_v[i] - pick(i, spread)).astype(jnp.bfloat16)
                total = jnp.sum(weight.astype(jnp.float32), axis=1, keepdims=True)
                sums = jnp.where(column == i, total, sums)
                strip = [
                    weight * owner_v[s, i : i + 1, :].astype(jnp.bfloat16)
                    for s in range(batch)
                ]
                strips.append(jnp.concatenate(strip, axis=0))
            weights = jnp.concatenate(strips, axis=1)
        weight_v[:, at * page : (at + count) * page] = weights
        more = attend(weights, 0, at, count)
        block = more if block is None else block + more
    totals = [
        jnp.where(across_v[s : s + 1, :] > 0.0, sums, 0.0) + owns[s]
        for s in range(batch)
    ]
    keep(0, block)

    def ship(source, target, send, recv, k, to):
        at = pl.ds(*pieces[k])
        return pltpu.make_async_remote_copy(
            src_ref=source.at[at],
            dst_ref=target.at[at],
            send_sem=send_sem.at[send],
            recv_sem=recv.at[k],
            device_id={"ctx": to},
            device_id_type=MESH,
        )

    def to_inbox(source, k):
        return ship(source, inbox, 0, out_recv, k, inward)

    def to_mid(k):
        return ship(part_v, inner_box, 0, in_recv, k, inward)

    def to_out(source, k):
        return ship(source, inner_box, 1, in_recv, k, outward)

    def stat_copy(to, origin, slot):
        return pltpu.make_async_remote_copy(
            src_ref=stat_out,
            dst_ref=stat_in.at[origin],
            send_sem=stat_send.at[slot],
            recv_sem=stat_recv.at[origin],
            device_id={"ctx": to},
            device_id_type=MESH,
        )

    def other(off):
        to = lax.rem(me + off, n)
        return to, (to > 0) & (to < n - 1)

    lane_row = lax.broadcasted_iota(jnp.int32, (rows, page), 1)
    for g in range(groups):
        pairs = [
            jnp.where(lane_row == 0, tops[s], jnp.sum(totals[s], axis=1, keepdims=True))
            for s in range(g * many, (g + 1) * many)
        ]
        tile = jnp.transpose(jnp.concatenate(pairs, axis=0))[0:8]
        stat_out[g] = tile
        stat_in[pl.ds(me, 1), g] = tile[None]

    pl.semaphore_wait(barrier, n - 1)

    @pl.loop(1, n)
    def _(off):
        to, wanted = other(off)

        @pl.when(wanted)
        def _():
            stat_copy(to, me, off).start()

    sent = 0
    for j in range(0, wide, group):
        if j > 0:
            block = None
            for at, count in tiles:
                weights = weight_v[:, at * page : (at + count) * page]
                more = attend(weights, j, at, count)
                block = more if block is None else block + more
            keep(j, block)
        ready = [
            k for k in range(sent, number) if sum(pieces[k]) <= (j + group) * height
        ]
        sent += len(ready)

        @pl.when(is_end)
        def _():
            for k in ready:
                to_inbox(acc_v, k).start()

    def emit(k, value):
        value = value.astype(jnp.bfloat16)
        first, size = pieces[k]
        lo = first
        while lo < first + size:
            j, at = divmod(lo, height)
            s, r = divmod(at, rows)
            take = min(rows - r, first + size - lo)
            out_ref[0, s, r : r + take, j * page : (j + 1) * page] = value[
                lo - first : lo - first + take
            ]
            lo += take

    def beyond(dist):
        return jnp.where(left, jnp.maximum(me - dist, 0), jnp.minimum(me + dist, n - 1))

    def turn(first, second):
        row = lax.broadcasted_iota(jnp.int32, (page, page), 0)
        turned = jnp.transpose(jnp.where(row == 0, first, second))
        return turned[:, 0:1], turned[:, 1:2]

    def part_factors(g):
        theirs = stat_in[pl.ds(beyond(1), 1), g, 0:1, :].reshape(1, page)
        for dist in range(2, half):
            theirs = jnp.maximum(
                theirs, stat_in[pl.ds(beyond(dist), 1), g, 0:1, :].reshape(1, page)
            )
        mine = stat_out[g, 0:1, :]
        best = jnp.maximum(mine, theirs)
        return turn(jnp.exp2(mine - best), jnp.exp2(theirs - best))

    def total_factors(g):
        tiles = [stat_in[j, g] for j in range(n)]
        low = functools.reduce(jnp.maximum, tiles[:half])[0:1]
        high = functools.reduce(jnp.maximum, tiles[half:])[0:1]
        best = jnp.maximum(low, high)
        denom = jnp.zeros((1, page), jnp.float32)
        for tile in tiles:
            denom = denom + jnp.exp2(tile[0:1] - best) * tile[1:2]
        low = jnp.exp2(low - best) / denom
        high = jnp.exp2(high - best) / denom
        return turn(jnp.where(left, low, high), jnp.where(left, high, low))

    def await_stats(wanted):
        @pl.loop(1, n)
        def _(off):
            origin = lax.rem(me + off, n)
            outer = jnp.where(left, origin < me, origin > me)

            @pl.when(outer == wanted)
            def _():
                stat_copy(me, origin, off).wait_recv()

    def rows_of(factor, k):
        first, size = pieces[k]
        parts = []
        lo = first
        while lo < first + size:
            at = lo % height
            take = min(height - at, first + size - lo)
            parts.append(factor[at : at + take])
            lo += take
        return parts[0] if len(parts) == 1 else jnp.concatenate(parts, axis=0)

    @pl.when(inner)
    def _():
        def scales(factors):
            pairs = [factors(g) for g in range(groups)]
            return [jnp.concatenate(f, axis=0) for f in zip(*pairs)]

        await_stats(True)
        part_scales = scales(part_factors)

        def walk(lag):
            total_scales = None
            for k, d in merge(pieces, lag):
                if k is not None:
                    at = pl.ds(*pieces[k])
                    mine, theirs = (rows_of(f, k) for f in part_scales)
                    to_inbox(acc_v, k).wait_recv()
                    part_v[at] = acc_v[at] * mine + inbox[at] * theirs
                    if all_mid:
                        to_mid(k).start()
                    else:

                        @pl.when(is_mid)
                        def _():
                            to_mid(k).start()

                        @pl.when(jnp.logical_not(is_mid))
                        def _():
                            to_inbox(part_v, k).start()

                else:
                    at = pl.ds(*pieces[d])
                    if total_scales is None:
                        await_stats(False)
                        total_scales = scales(total_factors)
                    mine, theirs = (rows_of(f, d) for f in total_scales)
                    to_mid(d).wait_recv()

                    def finish():
                        total = part_v[at] * mine + inner_box[at] * theirs
                        total_v[at] = total
                        to_out(total_v, d).start()
                        emit(d, total)

                    if all_mid:
                        finish()
                    else:
                        pl.when(is_mid)(finish)

                        @pl.when(jnp.logical_not(is_mid))
                        def _():
                            to_out(inner_box, d).start()
                            emit(d, inner_box[at])

        if LAG_LEFT == LAG_RIGHT:
            walk(LAG_LEFT)
        else:

            @pl.when(left)
            def _():
                walk(LAG_LEFT)

            @pl.when(jnp.logical_not(left))
            def _():
                walk(LAG_RIGHT)

        pltpu.make_async_remote_copy(
            src_ref=total_v,
            dst_ref=inner_box,
            send_sem=send_sem.at[1],
            recv_sem=in_recv.at[0],
            device_id={"ctx": outward},
            device_id_type=MESH,
        ).wait_send()

    @pl.when(is_end)
    def _():
        for k in range(number):
            to_mid(k).wait_recv()
            emit(k, inner_box[pl.ds(*pieces[k])])

    pltpu.make_async_remote_copy(
        src_ref=part_v,
        dst_ref=inbox,
        send_sem=send_sem.at[0],
        recv_sem=out_recv.at[0],
        device_id={"ctx": inward},
        device_id_type=MESH,
    ).wait_send()

    @pl.loop(1, n)
    def _(off):
        to, wanted = other(off)

        @pl.when(wanted)
        def _():
            stat_copy(to, me, off).wait_send()


def local(n, kv_cache, queries, new_latent, page_counts, page_tails, page_slots):
    _, pages, page, width = kv_cache.shape
    _, batch, rows, _ = queries.shape
    height = batch * rows
    flat = (LATENT // page * height, page)
    number = len(cut(flat[0]))
    groups = height // page
    hbm = pl.BlockSpec(memory_space=pltpu.HBM)
    dma = pltpu.SemaphoreType.DMA
    return pl.pallas_call(
        functools.partial(kernel, n),
        out_shape=pltpu.VMEM((1, batch, rows, LATENT), jnp.bfloat16),
        in_specs=[hbm] * 6,
        scratch_shapes=[
            pltpu.SMEM(page_counts.shape, jnp.int32),
            pltpu.SMEM(page_tails.shape, jnp.int32),
            pltpu.VMEM(page_slots.shape, jnp.int32),
            pltpu.VMEM(new_latent.shape, jnp.bfloat16),
            pltpu.VMEM((batch, rows, width), jnp.bfloat16),
            pltpu.VMEM((pages, width, page), jnp.bfloat16),
            pltpu.VMEM((page, width), jnp.bfloat16),
            pltpu.VMEM((pages, page), jnp.float32),
            pltpu.VMEM((batch, pages, page), jnp.float32),
            pltpu.VMEM((8, page), jnp.float32),
            pltpu.VMEM((pages, rows, page), jnp.float32),
            pltpu.VMEM((height, (pages + 1) * page), jnp.bfloat16),
            pltpu.VMEM(flat, jnp.float32),
            pltpu.VMEM(flat, jnp.float32),
            pltpu.VMEM(flat, jnp.float32),
            pltpu.VMEM(flat, jnp.float32),
            pltpu.VMEM(flat, jnp.float32),
            pltpu.VMEM((groups, 8, page), jnp.float32),
            pltpu.VMEM((n, groups, 8, page), jnp.float32),
            dma((4,)),
            dma,
            dma((CHUNKS,)),
            dma((n,)),
            dma((n,)),
            dma((2,)),
            dma((number,)),
            dma((number,)),
        ],
        compiler_params=pltpu.CompilerParams(
            collective_id=0, has_side_effects=True
        ),
    )(page_counts, page_tails, page_slots, new_latent, queries, jnp.swapaxes(kv_cache, 2, 3))


def solution(mesh):
    in_specs = (
        P(("groups", "rep"), "ctx", None, None),
        P(("groups", "rep"), None, "head", None),
        P(("groups", "rep"), None, None),
        P(("groups", "rep"), None),
        P(("groups", "rep"), None),
        P(("groups", "rep"), None),
    )
    out_specs = P(("groups", "rep"), None, "head", None)
    return jax.shard_map(
        functools.partial(local, mesh.shape["ctx"]),
        mesh=mesh,
        in_specs=in_specs,
        out_specs=out_specs,
        check_vma=False,
    )
```

```python
import functools
import math

import jax
import jax.numpy as jnp
from jax import lax
from jax.experimental import pallas as pl
from jax.experimental.pallas import tpu as pltpu
from jax.sharding import PartitionSpec as P

LATENT = 512
SCALE = 192.0 ** (-0.5) * math.log2(math.e)
NEG = -1e30
PIECE = 48
HEAD = (16,16)
TAIL = (16,16)
LAG_LEFT = 304
LAG_RIGHT = 352
CHUNKS = 2
MESH = pl.DeviceIdType.MESH


def cut(total):
    ends = sum(HEAD) + sum(TAIL)
    head, tail = (HEAD, TAIL) if total > ends else ((), ())
    sizes = list(head)
    while sum(sizes) + sum(tail) < total:
        sizes.append(min(PIECE, total - sum(sizes) - sum(tail)))
    sizes.extend(tail)
    return [(sum(sizes[:k]), size) for k, size in enumerate(sizes)]


def merge(pieces, lag):
    order = []
    k = d = 0
    while d < len(pieces):
        if k < len(pieces) and pieces[k][0] < pieces[d][0] + lag:
            order.append((k, None))
            k += 1
        else:
            order.append((None, d))
            d += 1
    return order


def kernel(
    n,
    counts_hbm,
    tails_hbm,
    slots_hbm,
    latent_hbm,
    q_hbm,
    kv_hbm,
    out_ref,
    counts_ref,
    tails_ref,
    slots_ref,
    latent_ref,
    q_v,
    kv_v,
    own_v,
    bias_v,
    owner_v,
    across_v,
    score_v,
    weight_v,
    acc_v,
    inbox,
    part_v,
    inner_box,
    total_v,
    stat_out,
    stat_in,
    small_sem,
    q_sem,
    kv_sem,
    stat_send,
    stat_recv,
    send_sem,
    out_recv,
    in_recv,
):
    batch, rows, width = q_v.shape
    pages, _, page = kv_v.shape
    tokens = pages * page
    slots = slots_ref.shape[1]
    height = batch * rows
    groups, many = stat_out.shape[0], page // rows
    wide = LATENT // page
    pieces = cut(wide * height)
    number = len(pieces)
    me = lax.axis_index("ctx")
    half = n // 2
    left = me < half
    inward = jnp.where(left, me + 1, me - 1)
    outward = jnp.where(left, me - 1, me + 1)
    is_end = (me == 0) | (me == n - 1)
    is_mid = (me == half - 1) | (me == half)
    inner = jnp.logical_not(is_end)
    all_mid = n <= 4

    smalls = [
        pltpu.make_async_copy(source, target, small_sem.at[i])
        for i, (source, target) in enumerate(
            [
                (counts_hbm, counts_ref),
                (tails_hbm, tails_ref),
                (slots_hbm, slots_ref),
                (latent_hbm, latent_ref),
            ]
        )
    ]
    for small in smalls:
        small.start()
    q_load = pltpu.make_async_copy(q_hbm.at[0], q_v, q_sem)
    q_load.start()
    step = pages // CHUNKS
    loads = []
    for i in range(CHUNKS):
        at = pl.ds(i * step, step)
        loads.append(
            pltpu.make_async_copy(kv_hbm.at[0, at], kv_v.at[at], kv_sem.at[i])
        )
        loads[-1].start(priority=1)

    barrier = pltpu.get_barrier_semaphore()

    @pl.loop(1, n)
    def _(off):
        pl.semaphore_signal(
            barrier, inc=1, device_id={"ctx": lax.rem(me + off, n)}, device_id_type=MESH
        )

    for small in smalls:
        small.wait()
    own_v[...] = jnp.zeros((page, width), jnp.bfloat16)
    own_v[0:batch, :] = latent_ref[0]

    slot_id = me * pages + lax.broadcasted_iota(jnp.int32, (pages, slots), 0)
    rank = lax.broadcasted_iota(jnp.int32, (pages, slots), 1)
    match = slots_ref[...] == slot_id
    lane = lax.broadcasted_iota(jnp.int32, (pages, page), 1)
    begin = jnp.int32(0)
    limits = jnp.zeros((pages, page), jnp.float32)
    table = jnp.zeros((pages, page), jnp.float32)
    for s in range(batch):
        count = counts_ref[0, s]
        length = (count - 1) * page + tails_ref[0, s]
        place = rank - begin
        inside = match & (place >= 0) & (place < count)
        limit = jnp.sum(
            jnp.where(inside, (length - place * page).astype(jnp.float32), 0.0),
            axis=1,
            keepdims=True,
        )
        limits = limits + limit
        table = jnp.where(lane == s, limit, table)
        owner_v[s, :, :] = jnp.where(limit > 0.0, jnp.ones((pages, page)), 0.0)
        begin = begin + count
    bias_v[...] = jnp.where(lane.astype(jnp.float32) < limits, 0.0, NEG)
    square = jnp.concatenate(
        [table, jnp.zeros((page - pages, page), jnp.float32)], axis=0
    )
    across_v[...] = jnp.transpose(square)[0:8]

    q_load.wait()
    queries = q_v[...].reshape(height, width)
    column = lax.broadcasted_iota(jnp.int32, (rows, page), 1)
    peaks = jnp.full((rows, page), NEG, jnp.float32)
    nt = (((1,), (1,)), ((), ()))

    def pick(at, parts):
        chosen = parts[-1]
        for s in reversed(range(batch - 1)):
            chosen = jnp.where(owner_v[s, at : at + 1, :] > 0.5, parts[s], chosen)
        return chosen

    def strips_of(block, j):
        cols = slice(j * page, (j + 1) * page)
        return [block[s * rows : (s + 1) * rows, cols] for s in range(batch)]

    block = lax.dot_general(queries, own_v[...], nt, preferred_element_type=jnp.float32)
    owns = [
        jnp.where((column == s) & (me == 0), strip * SCALE, NEG)
        for s, strip in enumerate(strips_of(block, 0))
    ]
    for first in range(0, pages, 2):
        two = min(2, pages - first)
        if first % step == 0:
            loads[first // step].wait()
        keys = jnp.concatenate([kv_v[first + j] for j in range(two)], axis=1)
        block = jnp.dot(queries, keys, preferred_element_type=jnp.float32)
        for j in range(two):
            at = first + j
            value = pick(at, strips_of(block, j)) * SCALE + bias_v[at : at + 1, :]
            score_v[at] = value
            peaks = jnp.where(
                column == at, jnp.max(value, axis=1, keepdims=True), peaks
            )

    tops = []
    for s in range(batch):
        held = jnp.where(across_v[s : s + 1, :] > 0.0, peaks, NEG)
        tops.append(jnp.max(jnp.maximum(held, owns[s]), axis=1, keepdims=True))
    spread = [jnp.broadcast_to(top, (rows, page)) for top in tops]
    sums = jnp.zeros((rows, page), jnp.float32)
    tiles = [(at, min(2, pages - at)) for at in range(0, pages, 2)] + [(pages, 1)]
    group = 2

    def attend(weights, first, at, count):
        span = slice(first * page, (first + group) * page)
        if at == pages:
            return jnp.dot(weights, own_v[:, span], preferred_element_type=jnp.float32)
        values = jnp.concatenate([kv_v[at + i, span, :] for i in range(count)], axis=1)
        return lax.dot_general(weights, values, nt, preferred_element_type=jnp.float32)

    def keep(first, block):
        for i in range(group):
            acc_v[(first + i) * height : (first + i + 1) * height, :] = block[
                :, i * page : (i + 1) * page
            ]

    block = None
    for at, count in tiles:
        if at == pages:
            strip = [
                jnp.exp2(own - top).astype(jnp.bfloat16)
                for own, top in zip(owns, spread)
            ]
            owns = [part.astype(jnp.float32) for part in strip]
            weights = jnp.concatenate(strip, axis=0)
        else:
            strips = []
            for i in range(at, at + count):
                weight = jnp.exp2(score_v[i] - pick(i, spread)).astype(jnp.bfloat16)
                total = jnp.sum(weight.astype(jnp.float32), axis=1, keepdims=True)
                sums = jnp.where(column == i, total, sums)
                strip = [
                    weight * owner_v[s, i : i + 1, :].astype(jnp.bfloat16)
                    for s in range(batch)
                ]
                strips.append(jnp.concatenate(strip, axis=0))
            weights = jnp.concatenate(strips, axis=1)
        weight_v[:, at * page : (at + count) * page] = weights
        more = attend(weights, 0, at, count)
        block = more if block is None else block + more
    totals = [
        jnp.where(across_v[s : s + 1, :] > 0.0, sums, 0.0) + owns[s]
        for s in range(batch)
    ]
    keep(0, block)

    def ship(source, target, send, recv, k, to):
        at = pl.ds(*pieces[k])
        return pltpu.make_async_remote_copy(
            src_ref=source.at[at],
            dst_ref=target.at[at],
            send_sem=send_sem.at[send],
            recv_sem=recv.at[k],
            device_id={"ctx": to},
            device_id_type=MESH,
        )

    def to_inbox(source, k):
        return ship(source, inbox, 0, out_recv, k, inward)

    def to_mid(k):
        return ship(part_v, inner_box, 0, in_recv, k, inward)

    def to_out(source, k):
        return ship(source, inner_box, 1, in_recv, k, outward)

    def stat_copy(to, origin, slot):
        return pltpu.make_async_remote_copy(
            src_ref=stat_out,
            dst_ref=stat_in.at[origin],
            send_sem=stat_send.at[slot],
            recv_sem=stat_recv.at[origin],
            device_id={"ctx": to},
            device_id_type=MESH,
        )

    def other(off):
        to = lax.rem(me + off, n)
        return to, (to > 0) & (to < n - 1)

    lane_row = lax.broadcasted_iota(jnp.int32, (rows, page), 1)
    for g in range(groups):
        pairs = [
            jnp.where(lane_row == 0, tops[s], jnp.sum(totals[s], axis=1, keepdims=True))
            for s in range(g * many, (g + 1) * many)
        ]
        tile = jnp.transpose(jnp.concatenate(pairs, axis=0))[0:8]
        stat_out[g] = tile
        stat_in[pl.ds(me, 1), g] = tile[None]

    pl.semaphore_wait(barrier, n - 1)

    @pl.loop(1, n)
    def _(off):
        to, wanted = other(off)

        @pl.when(wanted)
        def _():
            stat_copy(to, me, off).start()

    sent = 0
    for j in range(0, wide, group):
        if j > 0:
            block = None
            for at, count in tiles:
                weights = weight_v[:, at * page : (at + count) * page]
                more = attend(weights, j, at, count)
                block = more if block is None else block + more
            keep(j, block)
        ready = [
            k for k in range(sent, number) if sum(pieces[k]) <= (j + group) * height
        ]
        sent += len(ready)

        @pl.when(is_end)
        def _():
            for k in ready:
                to_inbox(acc_v, k).start()

    def emit(k, value):
        value = value.astype(jnp.bfloat16)
        first, size = pieces[k]
        lo = first
        while lo < first + size:
            j, at = divmod(lo, height)
            s, r = divmod(at, rows)
            take = min(rows - r, first + size - lo)
            out_ref[0, s, r : r + take, j * page : (j + 1) * page] = value[
                lo - first : lo - first + take
            ]
            lo += take

    def beyond(dist):
        return jnp.where(left, jnp.maximum(me - dist, 0), jnp.minimum(me + dist, n - 1))

    def turn(first, second):
        row = lax.broadcasted_iota(jnp.int32, (page, page), 0)
        turned = jnp.transpose(jnp.where(row == 0, first, second))
        return turned[:, 0:1], turned[:, 1:2]

    def part_factors(g):
        theirs = stat_in[pl.ds(beyond(1), 1), g, 0:1, :].reshape(1, page)
        for dist in range(2, half):
            theirs = jnp.maximum(
                theirs, stat_in[pl.ds(beyond(dist), 1), g, 0:1, :].reshape(1, page)
            )
        mine = stat_out[g, 0:1, :]
        best = jnp.maximum(mine, theirs)
        return turn(jnp.exp2(mine - best), jnp.exp2(theirs - best))

    def total_factors(g):
        tiles = [stat_in[j, g] for j in range(n)]
        low = functools.reduce(jnp.maximum, tiles[:half])[0:1]
        high = functools.reduce(jnp.maximum, tiles[half:])[0:1]
        best = jnp.maximum(low, high)
        denom = jnp.zeros((1, page), jnp.float32)
        for tile in tiles:
            denom = denom + jnp.exp2(tile[0:1] - best) * tile[1:2]
        low = jnp.exp2(low - best) / denom
        high = jnp.exp2(high - best) / denom
        return turn(jnp.where(left, low, high), jnp.where(left, high, low))

    def await_stats(wanted):
        @pl.loop(1, n)
        def _(off):
            origin = lax.rem(me + off, n)
            outer = jnp.where(left, origin < me, origin > me)

            @pl.when(outer == wanted)
            def _():
                stat_copy(me, origin, off).wait_recv()

    def rows_of(factor, k):
        first, size = pieces[k]
        parts = []
        lo = first
        while lo < first + size:
            at = lo % height
            take = min(height - at, first + size - lo)
            parts.append(factor[at : at + take])
            lo += take
        return parts[0] if len(parts) == 1 else jnp.concatenate(parts, axis=0)

    @pl.when(inner)
    def _():
        def scales(factors):
            pairs = [factors(g) for g in range(groups)]
            return [jnp.concatenate(f, axis=0) for f in zip(*pairs)]

        await_stats(True)
        part_scales = scales(part_factors)

        def walk(lag):
            total_scales = None
            for k, d in merge(pieces, lag):
                if k is not None:
                    at = pl.ds(*pieces[k])
                    mine, theirs = (rows_of(f, k) for f in part_scales)
                    to_inbox(acc_v, k).wait_recv()
                    part_v[at] = acc_v[at] * mine + inbox[at] * theirs
                    if all_mid:
                        to_mid(k).start()
                    else:

                        @pl.when(is_mid)
                        def _():
                            to_mid(k).start()

                        @pl.when(jnp.logical_not(is_mid))
                        def _():
                            to_inbox(part_v, k).start()

                else:
                    at = pl.ds(*pieces[d])
                    if total_scales is None:
                        await_stats(False)
                        total_scales = scales(total_factors)
                    mine, theirs = (rows_of(f, d) for f in total_scales)
                    to_mid(d).wait_recv()

                    def finish():
                        total = part_v[at] * mine + inner_box[at] * theirs
                        total_v[at] = total
                        to_out(total_v, d).start()
                        emit(d, total)

                    if all_mid:
                        finish()
                    else:
                        pl.when(is_mid)(finish)

                        @pl.when(jnp.logical_not(is_mid))
                        def _():
                            to_out(inner_box, d).start()
                            emit(d, inner_box[at])

        if LAG_LEFT == LAG_RIGHT:
            walk(LAG_LEFT)
        else:

            @pl.when(left)
            def _():
                walk(LAG_LEFT)

            @pl.when(jnp.logical_not(left))
            def _():
                walk(LAG_RIGHT)

        pltpu.make_async_remote_copy(
            src_ref=total_v,
            dst_ref=inner_box,
            send_sem=send_sem.at[1],
            recv_sem=in_recv.at[0],
            device_id={"ctx": outward},
            device_id_type=MESH,
        ).wait_send()

    @pl.when(is_end)
    def _():
        for k in range(number):
            to_mid(k).wait_recv()
            emit(k, inner_box[pl.ds(*pieces[k])])

    pltpu.make_async_remote_copy(
        src_ref=part_v,
        dst_ref=inbox,
        send_sem=send_sem.at[0],
        recv_sem=out_recv.at[0],
        device_id={"ctx": inward},
        device_id_type=MESH,
    ).wait_send()

    @pl.loop(1, n)
    def _(off):
        to, wanted = other(off)

        @pl.when(wanted)
        def _():
            stat_copy(to, me, off).wait_send()


def local(n, kv_cache, queries, new_latent, page_counts, page_tails, page_slots):
    _, pages, page, width = kv_cache.shape
    _, batch, rows, _ = queries.shape
    height = batch * rows
    flat = (LATENT // page * height, page)
    number = len(cut(flat[0]))
    groups = height // page
    hbm = pl.BlockSpec(memory_space=pltpu.HBM)
    dma = pltpu.SemaphoreType.DMA
    return pl.pallas_call(
        functools.partial(kernel, n),
        out_shape=pltpu.VMEM((1, batch, rows, LATENT), jnp.bfloat16),
        in_specs=[hbm] * 6,
        scratch_shapes=[
            pltpu.SMEM(page_counts.shape, jnp.int32),
            pltpu.SMEM(page_tails.shape, jnp.int32),
            pltpu.VMEM(page_slots.shape, jnp.int32),
            pltpu.VMEM(new_latent.shape, jnp.bfloat16),
            pltpu.VMEM((batch, rows, width), jnp.bfloat16),
            pltpu.VMEM((pages, width, page), jnp.bfloat16),
            pltpu.VMEM((page, width), jnp.bfloat16),
            pltpu.VMEM((pages, page), jnp.float32),
            pltpu.VMEM((batch, pages, page), jnp.float32),
            pltpu.VMEM((8, page), jnp.float32),
            pltpu.VMEM((pages, rows, page), jnp.float32),
            pltpu.VMEM((height, (pages + 1) * page), jnp.bfloat16),
            pltpu.VMEM(flat, jnp.float32),
            pltpu.VMEM(flat, jnp.float32),
            pltpu.VMEM(flat, jnp.float32),
            pltpu.VMEM(flat, jnp.float32),
            pltpu.VMEM(flat, jnp.float32),
            pltpu.VMEM((groups, 8, page), jnp.float32),
            pltpu.VMEM((n, groups, 8, page), jnp.float32),
            dma((4,)),
            dma,
            dma((CHUNKS,)),
            dma((n,)),
            dma((n,)),
            dma((2,)),
            dma((number,)),
            dma((number,)),
        ],
        compiler_params=pltpu.CompilerParams(
            collective_id=0, has_side_effects=True
        ),
    )(page_counts, page_tails, page_slots, new_latent, queries, jnp.swapaxes(kv_cache, 2, 3))


def solution(mesh):
    in_specs = (
        P(("groups", "rep"), "ctx", None, None),
        P(("groups", "rep"), None, "head", None),
        P(("groups", "rep"), None, None),
        P(("groups", "rep"), None),
        P(("groups", "rep"), None),
        P(("groups", "rep"), None),
    )
    out_specs = P(("groups", "rep"), None, "head", None)
    return jax.shard_map(
        functools.partial(local, mesh.shape["ctx"]),
        mesh=mesh,
        in_specs=in_specs,
        out_specs=out_specs,
        check_vma=False,
    )
```
